32 devices in a mesh: gx: 4 (over x, core), gy: 2 (over y), gz: 4 (over z).
Axes of the slice: x: 2, y: 2, z: 4, core: 2. Of those that a mesh axis runs over, the one named last changes fastest.
Arguments:
- coef: float32 [4, 64, 64, 512], P(None, 'gx', 'gy', 'gz'), may hold values from -6 to 6
- keep: int32 [4, 16, 16, 128], P(None, 'gx', 'gy', 'gz'), may hold values from 1 to 10
- courant: float32 [64, 64, 512], P('gx', 'gy', 'gz'), may hold values from 0.05 to 0.2
- damp: float32 [64, 64, 512], P('gx', 'gy', 'gz'), may hold values from 0 to 0.3
- adj_next: float32 [64, 64, 512], P('gx', 'gy', 'gz'), may hold values from -6 to 6
- adj_now: float32 [64, 64, 512], P('gx', 'gy', 'gz'), may hold values from -6 to 6
- rec_cell: int32 [4, 2, 4, 128], P('gx', 'gy', 'gz'), may hold values from 0 to 65535
- rec_data: float32 [4, 2, 4, 4, 128], P('gx', 'gy', 'gz'), may hold values from -6 to 6
Outputs:
- gradient: float32 [64, 64, 512], P('gx', 'gy', 'gz')
- adjoint_last: float32 [64, 64, 512], P('gx', 'gy', 'gz')
- adjoint_before: float32 [64, 64, 512], P('gx', 'gy', 'gz')
The draws below stay inside these ranges and needn't reach their ends.
Inputs may be any that keep to these rules, and one draw needn't show every extreme that they name: `keep`: A block's coefficient (a, b, c) is kept when a + b + c is below this count. `rec_cell`: A row-major index into the 16 x 32 x 128 cells of the device's own block; indices may repeat.
All inputs are finite; a program needn't handle non-finite values.
Results may differ from the reference program's by a relative error of at most 0.00013.
Values sent between devices are 32-bit elements; how exact they have to be, the bound alone decides.
A program may use at most 64 MiB of HBM per device.

```python
import math
import jax
import jax.numpy as jnp
from jax import lax

CX = 16
CY = 32
CZ = 128
RECS = 128
STEPS = 4
NX = 64
NY = 64
NZ = 512
N_GX = 4
N_GY = 2
N_GZ = 4


def set_ends(array, own_key, low, high):
    spot = [jax.random.randint(jax.random.fold_in(own_key, axis), (), 0, length) for axis, length in enumerate(array.shape)]
    widest = array.shape.index(max(array.shape))
    next_to = spot[:widest] + [(spot[widest] + 1) % array.shape[widest]] + spot[widest + 1:]
    return array.at[tuple(spot)].set(low).at[tuple(next_to)].set(high)


def block_scale(stream_key, dims, split, least, high):
    level = 1.0
    for axis_at, blocks in split:
        steps = jax.random.uniform(jax.random.fold_in(jax.random.fold_in(stream_key, 6), axis_at), (blocks,), jnp.float32, least / len(split), high / len(split))
        level = level * jnp.repeat(jnp.exp(steps), dims[axis_at] // blocks).reshape((-1,) + (1,) * (len(dims) - 1 - axis_at))
    return level


def scatter_about(stream_key, shape, deviation, limit, split=(), kind=jnp.bfloat16):
    entries = deviation * jax.random.normal(stream_key, shape, jnp.float32)
    if split:
        entries = entries * block_scale(stream_key, shape, split, -0.22, 0.18)
    return jnp.clip(entries, -limit, limit).astype(kind)


def setup_inputs(seed: int = 0) -> dict:
    key_of = jax.random.split(jax.random.key(seed), 9)
    coef = scatter_about(key_of[0], (STEPS, NX, NY, NZ), 1.0, 6.0, ((1, 4), (2, 2), (3, 4)), jnp.float32)
    keep = set_ends(jax.random.randint(key_of[1], (STEPS, NX // 4, NY // 4, NZ // 4), 1, 11), jax.random.fold_in(key_of[1], 1), 1, 10).astype(jnp.int32)
    courant = jnp.clip(jnp.exp(math.log(0.2) - 1.3862944 * jax.random.uniform(key_of[2], (NX, NY, NZ), jnp.float32) ** block_scale(key_of[2], (NX, NY, NZ), ((0, 4), (1, 2), (2, 4)), -0.2, 0.2)), 0.05, 0.2)
    damp = jnp.clip(0.3 * jax.random.uniform(key_of[3], (NX, NY, NZ), jnp.float32) ** block_scale(key_of[3], (NX, NY, NZ), ((0, 4), (1, 2), (2, 4)), -0.2, 0.2), 0.0, 0.3)
    adj_next = scatter_about(key_of[4], (NX, NY, NZ), 1.0, 6.0, ((0, 4), (1, 2), (2, 4)), jnp.float32)
    adj_now = scatter_about(key_of[5], (NX, NY, NZ), 1.0, 6.0, ((0, 4), (1, 2), (2, 4)), jnp.float32)
    rec_cell = set_ends(jax.random.randint(key_of[6], (N_GX, N_GY, N_GZ, RECS), 0, CX * CY * CZ), jax.random.fold_in(key_of[6], 1), 0, (CX * CY * CZ) - 1).astype(jnp.int32)
    rec_data = scatter_about(key_of[7], (N_GX, N_GY, N_GZ, STEPS, RECS), 1.0, 6.0, ((0, 4), (1, 2), (2, 4)), jnp.float32)
    return dict(coef=coef, keep=keep, courant=courant, damp=damp, adj_next=adj_next, adj_now=adj_now, rec_cell=rec_cell, rec_data=rec_data)


STAR = (-205.0 / 72.0, 8.0 / 5.0, -1.0 / 5.0, 8.0 / 315.0, -1.0 / 560.0)

def dct_table():
    freq = jnp.arange(4, dtype=jnp.float32)[:, None]
    place = jnp.arange(4, dtype=jnp.float32)[None, :]
    scales = jnp.where(freq == 0.0, 0.5, jnp.sqrt(jnp.float32(0.5)))
    return scales * jnp.cos(jnp.pi * (2.0 * place + 1.0) * freq / 8.0)

def decode(block_coef, block_keep):
    levels = (jnp.arange(NX, dtype=jnp.int32) % 4)[:, None, None] + (jnp.arange(NY, dtype=jnp.int32) % 4)[None, :, None] + (jnp.arange(NZ, dtype=jnp.int32) % 4)[None, None, :]
    spread = jnp.repeat(jnp.repeat(jnp.repeat(block_keep, 4, axis=0), 4, axis=1), 4, axis=2)
    masked = jnp.where(levels < spread, block_coef, 0.0)
    shaped = masked.reshape(NX // 4, 4, NY // 4, 4, NZ // 4, 4)
    table = dct_table()
    out = jnp.einsum('xaybzc,ai,bj,ck->xiyjzk', shaped, table, table, table, precision=lax.Precision.HIGHEST)
    return out.reshape(NX, NY, NZ)

def laplace(field):
    padded = jnp.pad(field, 4)
    size_x, size_y, size_z = field.shape
    total = 3.0 * STAR[0] * field
    for reach in range(1, 5):
        plus_x = padded[4 + reach:4 + reach + size_x, 4:4 + size_y, 4:4 + size_z]
        minus_x = padded[4 - reach:4 - reach + size_x, 4:4 + size_y, 4:4 + size_z]
        plus_y = padded[4:4 + size_x, 4 + reach:4 + reach + size_y, 4:4 + size_z]
        minus_y = padded[4:4 + size_x, 4 - reach:4 - reach + size_y, 4:4 + size_z]
        plus_z = padded[4:4 + size_x, 4:4 + size_y, 4 + reach:4 + reach + size_z]
        minus_z = padded[4:4 + size_x, 4:4 + size_y, 4 - reach:4 - reach + size_z]
        total = total + STAR[reach] * (plus_x + minus_x + plus_y + minus_y + plus_z + minus_z)
    return total

def reference(coef, keep, courant, damp, adj_next, adj_now, rec_cell, rec_data):
    local_x = rec_cell // (CY * CZ)
    local_y = rec_cell // CZ % CY
    local_z = rec_cell % CZ
    global_x = jnp.arange(N_GX, dtype=jnp.int32)[:, None, None, None] * CX + local_x
    global_y = jnp.arange(N_GY, dtype=jnp.int32)[None, :, None, None] * CY + local_y
    global_z = jnp.arange(N_GZ, dtype=jnp.int32)[None, None, :, None] * CZ + local_z
    flat = ((global_x * NY + global_y) * NZ + global_z).reshape(-1).astype(jnp.int32)
    gradient = jnp.zeros((NX, NY, NZ), jnp.float32)
    later = adj_next
    current = adj_now
    for step in range(STEPS):
        forward = decode(coef[step], keep[step])
        gradient = gradient + courant * current * laplace(forward)
        inject = jnp.zeros((NX * NY * NZ,), jnp.float32).at[flat].add(rec_data[:, :, :, step, :].reshape(-1)).reshape(NX, NY, NZ)
        earlier = (2.0 * current - (1.0 - damp) * later + courant * laplace(current) + inject) / (1.0 + damp)
        later = current
        current = earlier
    return (gradient, current, later)
```

```python
import functools

import jax
import jax.numpy as jnp
import numpy as np
from jax import lax
from jax.experimental import pallas as pl
from jax.experimental.pallas import tpu as pltpu
from jax.sharding import PartitionSpec as P

STAR = (-205.0 / 72.0, 8.0 / 5.0, -1.0 / 5.0, 8.0 / 315.0, -1.0 / 560.0)
MESH = pl.DeviceIdType.MESH
F32, BF16 = jnp.float32, jnp.bfloat16
AXES = ("gx", "gy", "gz")
PADX, PADY = 4, 8


def halves_np(table):
    high = table.astype(jnp.bfloat16)
    low = (table - high.astype(np.float32)).astype(jnp.bfloat16)
    return high, low


def tables(size_y, size_z):
    freq, place = np.arange(4)[:, None], np.arange(4)[None, :]
    scale = np.where(freq == 0, 0.5, np.sqrt(0.5))
    dct = scale * np.cos(np.pi * (2.0 * place + 1.0) * freq / 8.0)
    dz = np.kron(np.eye(size_z // 4), dct).astype(np.float32)
    dxy = np.kron(dct, np.kron(np.eye(size_y // 4), dct)).T.astype(np.float32)
    taps = {k: STAR[k] for k in range(1, 5)}
    inner = np.zeros((size_z, size_z), np.float32)
    halo = np.zeros((8, size_z), np.float32)
    for lane in range(size_z):
        for k, c in taps.items():
            for at in (lane + k, lane - k):
                if 0 <= at < size_z:
                    inner[at, lane] += c
                elif at < 0:
                    halo[4 + at, lane] += c
                else:
                    halo[4 + at - size_z, lane] += c
    pick = np.zeros((8, size_z), np.float32)
    for j in range(4):
        pick[j, j] = 1.0
        pick[4 + j, size_z - 4 + j] = 1.0
    dz_h, dz_l = halves_np(dz)
    dxy_h, dxy_l = halves_np(dxy)
    in_h, in_l = halves_np(inner)
    ha_h, ha_l = halves_np(halo)
    pick = pick.astype(jnp.bfloat16)
    spread = np.kron(np.eye(size_z // 4), np.ones((1, 4))).astype(jnp.bfloat16)
    repeat = np.kron(np.eye(size_y // 4), np.ones((4, 1)))
    return (
        np.concatenate([dz_h, dz_h, dz_l], 0),
        np.concatenate([dxy_h, dxy_h, dxy_l], 1),
        np.concatenate([in_h, in_h, in_l], 0),
        np.concatenate([ha_h, ha_h, ha_l, 0 * ha_l], 0),
        np.concatenate([pick, pick], 1),
        spread,
        repeat,
    )


def halves(value):
    high = value.astype(BF16)
    low = (value - high.astype(F32)).astype(BF16)
    return high, low


def dot(a, b, dims=((1,), (0,))):
    return lax.dot_general(a, b, (dims, ((), ())), preferred_element_type=F32)


def kernel(shape, steps, ntab, *refs):
    size_x, size_y, size_z = shape
    rows = size_x * size_y
    groups = size_x // 4
    ins, refs = refs[:8 + ntab], refs[8 + ntab:]
    outs, refs = refs[:3], refs[3:]
    vins, refs = refs[:8 + ntab], refs[8 + ntab:]
    (F, X, Y, ZS, ZR, Z, J, INV, B, A, G, T, LAST, LF, isem, osem, ssem, rsem) = refs
    coef_v, keep_v, cour_v, damp_v, next_v, _, cell_v, data_v = vins[:8]
    dz_v, dxy_v, in_v, ha_v, pick_v, spread_v, repeat_v = vins[8:]
    pos = [lax.axis_index(a) for a in AXES]
    num = [lax.axis_size(a) for a in AXES]
    below = [p > 0 for p in pos]
    above = [p < n - 1 for p, n in zip(pos, num)]
    body = (pl.ds(PADX, size_x), pl.ds(PADY, size_y))

    order = [5, 3, 2, 4] + list(range(8, 8 + ntab)) + [6, 7, 1, 0]
    loads = {}
    for i in order:
        dst = F.at[(0,) + body] if i == 5 else vins[i]
        loads[i] = pltpu.make_async_copy(ins[i], dst, isem.at[i])
        loads[i].start()

    barrier = pltpu.get_barrier_semaphore()
    total = jnp.int32(0)
    for d, axis in enumerate(AXES):
        for has, to in ((above[d], pos[d] + 1), (below[d], pos[d] - 1)):
            total = total + has.astype(jnp.int32)

            @pl.when(has)
            def _(axis=axis, to=to):
                pl.semaphore_signal(barrier, inc=1, device_id={axis: to}, device_id_type=MESH)

    F[:, :, pl.ds(0, PADY), :] = jnp.zeros((2 * steps, size_x + 8, PADY, size_z), F32)
    F[:, :, pl.ds(PADY + size_y, PADY), :] = jnp.zeros((2 * steps, size_x + 8, PADY, size_z), F32)
    F[:, pl.ds(0, PADX), pl.ds(PADY, size_y), :] = jnp.zeros((2 * steps, PADX, size_y, size_z), F32)
    F[:, pl.ds(PADX + size_x, PADX), pl.ds(PADY, size_y), :] = jnp.zeros((2 * steps, PADX, size_y, size_z), F32)
    Y[:, 0, :, pl.ds(8, 8), :] = jnp.zeros((2 * steps, size_x, 8, size_z), F32)
    Y[:, 1, :, pl.ds(0, 8), :] = jnp.zeros((2 * steps, size_x, 8, size_z), F32)
    for side, has in ((0, below), (1, above)):

        @pl.when(jnp.logical_not(has[0]))
        def _(side=side):
            X[:, side] = jnp.zeros((2 * steps, 4, size_y, size_z), F32)

        @pl.when(jnp.logical_not(has[1]))
        def _(side=side):
            Y[:, side, :, pl.ds(4 + 4 * side, 4), :] = jnp.zeros((2 * steps, size_x, 4, size_z), F32)

        @pl.when(jnp.logical_not(has[2]))
        def _(side=side):
            ZR[:, side] = jnp.zeros((2 * steps, 4, rows), F32)

    def copy_of(r, d):
        axis, up = AXES[d // 2], d % 2 == 0
        if d == 0:
            src, dst = F.at[r, pl.ds(PADX + size_x - 4, 4), pl.ds(PADY, size_y)], X.at[r, 0]
        elif d == 1:
            src, dst = F.at[r, pl.ds(PADX, 4), pl.ds(PADY, size_y)], X.at[r, 1]
        elif d == 2:
            src = F.at[r, pl.ds(PADX, size_x), pl.ds(PADY + size_y - 4, 4)]
            dst = Y.at[r, 0, :, pl.ds(4, 4)]
        elif d == 3:
            src, dst = F.at[r, pl.ds(PADX, size_x), pl.ds(PADY, 4)], Y.at[r, 1, :, pl.ds(8, 4)]
        elif d == 4:
            src, dst = ZS.at[r, 1], ZR.at[r, 0]
        else:
            src, dst = ZS.at[r, 0], ZR.at[r, 1]
        to = pos[d // 2] + (1 if up else -1)
        return pltpu.make_async_remote_copy(
            src_ref=src, dst_ref=dst, send_sem=ssem.at[r, d], recv_sem=rsem.at[r, d],
            device_id={axis: to}, device_id_type=MESH,
        )

    def goes(d):
        return above[d // 2] if d % 2 == 0 else below[d // 2]

    def comes(d):
        return below[d // 2] if d % 2 == 0 else above[d // 2]

    def send(r, ds):
        for d in ds:

            @pl.when(goes(d))
            def _(d=d):
                copy_of(r, d).start()

    def arrive(r):
        for d in range(6):

            @pl.when(comes(d))
            def _(d=d):
                copy_of(r, d).wait_recv()

    def split_field(r):
        parts = [F[r, PADX + x, pl.ds(PADY, size_y), :] for x in range(size_x)]
        return halves(jnp.concatenate(parts, 0))

    def pack(r, high, low):
        packed = dot(pick_v[...], jnp.concatenate([high, low], 1), ((1,), (1,)))
        ZS[r, 0] = packed[0:4]
        ZS[r, 1] = packed[4:8]

    def inner_z(high, low):
        Z[...] = dot(jnp.concatenate([high, low, high], 1), in_v[...])

    def planes(fun, unit=2):
        def trip(i, carry):
            for j in range(unit):
                fun(i * unit + j)
            return carry

        lax.fori_loop(0, size_x // unit, trip, 0)

    def star(r, x):
        centre = pl.ds(PADY, size_y)
        out = 3.0 * STAR[0] * F[r, PADX + x, centre, :]
        for k in range(1, 5):
            out += STAR[k] * (
                (F[r, PADX + x + k, centre, :] + F[r, PADX + x - k, centre, :])
                + (F[r, PADX + x, pl.ds(PADY + k, size_y), :] + F[r, PADX + x, pl.ds(PADY - k, size_y), :])
            )
        return out + Z[pl.ds(pl.multiple_of(x * size_y, size_y), size_y), :]

    def halo_z(r):
        high, low = halves(jnp.concatenate([ZR[r, 0], ZR[r, 1]], 0).T)
        stacked = jnp.concatenate([high, low, high, jnp.zeros_like(low)], 1)
        Z[...] = dot(stacked, ha_v[...])

    def halo(r, x):
        out = Z[pl.ds(x * size_y, size_y), :]
        for k in range(1, 5):
            if x - k < 0:
                out += STAR[k] * X[r, 0, 4 + x - k]
            if x + k >= size_x:
                out += STAR[k] * X[r, 1, x + k - size_x]
        first = sum(STAR[k] * Y[r, 0, x, pl.ds(8 - k, 8), :] for k in range(1, 5))
        final = sum(STAR[k] * Y[r, 1, x, pl.ds(k, 8), :] for k in range(1, 5))
        return jnp.concatenate([out[0:8] + first, out[8:size_y - 8], out[size_y - 8:] + final], 0)

    cell = []

    def inject(s):
        if not cell:
            loads[6].wait()
            loads[7].wait()
        shift = size_z.bit_length() - 1
        at = cell_v[...]
        row = lax.shift_right_logical(at, jnp.full_like(at, shift))
        lane = at & (size_z - 1)
        hot = jnp.where(lax.broadcasted_iota(jnp.int32, (size_z, at.shape[1]), 0) == lane, 1.0, 0.0).astype(BF16)
        cell.append(1)
        spot = jnp.where(lax.broadcasted_iota(jnp.int32, (rows, at.shape[1]), 0) == row, data_v[pl.ds(s, 1), :], 0.0)
        high, low = halves(spot)
        J[...] = dot(jnp.concatenate([high, low], 1), jnp.concatenate([hot, hot], 1), ((1,), (1,)))

    def before_halo(s):
        def one(x):
            lap = star(s, x)
            later = next_v[x] if s == 0 else F[s - 1, PADX + x, pl.ds(PADY, size_y), :]
            got = J[pl.ds(pl.multiple_of(x * size_y, size_y), size_y), :]
            value = 2.0 * F[s, PADX + x, pl.ds(PADY, size_y), :] - (1.0 - damp_v[x]) * later + got
            A[x] = INV[x] * value + B[x] * lap

        planes(one)

    def after_halo(s):
        halo_z(s)
        for x in range(size_x):
            value = A[x] + B[x] * halo(s, x)
            if s == steps - 1:
                LAST[x] = value
            else:
                F[s + 1, PADX + x, pl.ds(PADY, size_y), :] = value

    def mask_setup():
        loads[1].wait()
        wide = dot(keep_v[...].astype(F32).astype(BF16), spread_v[...])
        sub = lax.broadcasted_iota(jnp.int32, (size_y, size_z), 0) % 4
        lan = lax.broadcasted_iota(jnp.int32, (size_y, size_z), 1) % 4
        level = (sub + lan).astype(F32)
        per = size_y // 4
        for g in range(steps * groups):
            T[g] = dot(repeat_v[...], wide[g * per:(g + 1) * per].astype(BF16)) - level

    def decode(s):
        r = steps + s
        parts = []
        for g in range(groups):
            limit = T[s * groups + g]
            for a in range(4):
                block = coef_v[s, g * 4 + a]
                parts.append(jnp.where(limit > float(a), block, 0.0))
        high, low = halves(jnp.concatenate(parts, 0))
        along = dot(jnp.concatenate([high, low, high], 1), dz_v[...])
        high, low = halves(along)
        span = 4 * size_y
        hs = jnp.concatenate([high[g * span:(g + 1) * span] for g in range(groups)], 1)
        ls = jnp.concatenate([low[g * span:(g + 1) * span] for g in range(groups)], 1)
        out = dot(dxy_v[...], jnp.concatenate([hs, ls, hs], 0))
        for g in range(groups):
            for a in range(4):
                F[r, PADX + 4 * g + a, pl.ds(PADY, size_y), :] = out[
                    a * size_y:(a + 1) * size_y, g * size_z:(g + 1) * size_z
                ]
        send(r, (0, 1, 2, 3))
        pack(r, *split_field(r))
        send(r, (4, 5))

    def gradient(s):
        r = steps + s
        inner_z(*split_field(r))

        def one(x):
            LF[x] = star(r, x)

        planes(one)
        arrive(r)
        halo_z(r)
        for x in range(size_x):
            term = cour_v[x] * F[s, PADX + x, pl.ds(PADY, size_y), :] * (LF[x] + halo(r, x))
            G[x] = term if s == 0 else G[x] + term

    def setup_scales():
        loads[2].wait()
        loads[3].wait()

        def one(x):
            inverse = 1.0 / (1.0 + damp_v[x])
            INV[x] = inverse
            B[x] = cour_v[x] * inverse

        planes(one)

    for i in (5,) + tuple(range(8, 8 + ntab)):
        loads[i].wait()
    high, low = split_field(0)
    pack(0, high, low)
    pl.semaphore_wait(barrier, total)
    send(0, range(6))
    writes = []
    for s in range(steps):
        inner_z(high, low)
        inject(s)
        if s == 0:
            setup_scales()
            loads[4].wait()
        before_halo(s)
        if s == 0:
            mask_setup()
            loads[0].wait()
        for t in (2 * s, 2 * s + 1):
            if t < steps:
                decode(t)
            elif t < 2 * steps:
                gradient(t - steps)
        if s == steps - 1:
            writes.append(pltpu.make_async_copy(F.at[(s,) + body], outs[2], osem.at[2]))
            writes.append(pltpu.make_async_copy(G, outs[0], osem.at[0]))
            for w in writes:
                w.start()
        arrive(s)
        after_halo(s)
        if s < steps - 1:
            send(s + 1, (0, 1, 2, 3))
            high, low = split_field(s + 1)
            pack(s + 1, high, low)
            send(s + 1, (4, 5))
    writes.append(pltpu.make_async_copy(LAST, outs[1], osem.at[1]))
    writes[-1].start()
    for r in range(2 * steps):
        for d in range(6):

            @pl.when(goes(d))
            def _(r=r, d=d):
                copy_of(r, d).wait_send()
    for w in writes:
        w.wait()


def local(coef, keep, courant, damp, adj_next, adj_now, rec_cell, rec_data):
    shape = adj_now.shape
    size_x, size_y, size_z = shape
    steps = coef.shape[0]
    rows = size_x * size_y
    args = [
        coef, keep.reshape(-1, keep.shape[-1]), courant, damp, adj_next, adj_now,
        rec_cell.reshape(1, -1), rec_data.reshape(steps, -1),
    ]
    tabs = list(tables(size_y, size_z))
    tabs[-1] = tabs[-1].astype(jnp.bfloat16)
    tabs = [jnp.asarray(t) for t in tabs]
    args += tabs
    box = pltpu.VMEM(shape, F32)
    flat = pltpu.VMEM((rows, size_z), F32)
    scratch = [pltpu.VMEM(a.shape, a.dtype) for a in args]
    scratch[5] = pltpu.VMEM((8, 128), F32)
    scratch += [
        pltpu.VMEM((2 * steps, size_x + 8, size_y + 16, size_z), F32),
        pltpu.VMEM((2 * steps, 2, 4, size_y, size_z), F32),
        pltpu.VMEM((2 * steps, 2, size_x, 16, size_z), F32),
        pltpu.VMEM((2 * steps, 2, 4, rows), F32),
        pltpu.VMEM((2 * steps, 2, 4, rows), F32),
        flat, flat, box, box, box, box,
        pltpu.VMEM((steps * size_x // 4, size_y, size_z), F32),
        box, box,
        pltpu.SemaphoreType.DMA((len(args),)),
        pltpu.SemaphoreType.DMA((3,)),
        pltpu.SemaphoreType.DMA((2 * steps, 6)),
        pltpu.SemaphoreType.DMA((2 * steps, 6)),
    ]
    hbm = pl.BlockSpec(memory_space=pl.ANY)
    return tuple(pl.pallas_call(
        functools.partial(kernel, shape, steps, len(tabs)),
        out_shape=[jax.ShapeDtypeStruct(shape, F32)] * 3,
        in_specs=[hbm] * len(args),
        out_specs=[hbm] * 3,
        scratch_shapes=scratch,
        compiler_params=pltpu.CompilerParams(
            collective_id=0, has_side_effects=True, vmem_limit_bytes=48 * 2**20
        ),
    )(*args))


def solution(mesh):
    in_specs = (
        P(None, "gx", "gy", "gz"),
        P(None, "gx", "gy", "gz"),
        P("gx", "gy", "gz"),
        P("gx", "gy", "gz"),
        P("gx", "gy", "gz"),
        P("gx", "gy", "gz"),
        P("gx", "gy", "gz", None),
        P("gx", "gy", "gz", None, None),
    )
    out_specs = (P("gx", "gy", "gz"), P("gx", "gy", "gz"), P("gx", "gy", "gz"))
    return jax.shard_map(local, mesh=mesh, in_specs=in_specs, out_specs=out_specs, check_vma=False)
```

```python
import functools

import jax
import jax.numpy as jnp
import numpy as np
from jax import lax
from jax.experimental import pallas as pl
from jax.experimental.pallas import tpu as pltpu
from jax.sharding import PartitionSpec as P

STAR = (-205.0 / 72.0, 8.0 / 5.0, -1.0 / 5.0, 8.0 / 315.0, -1.0 / 560.0)
MESH = pl.DeviceIdType.MESH
F32, BF16 = jnp.float32, jnp.bfloat16
AXES = ("gx", "gy", "gz")
PADX, PADY = 4, 8


def halves_np(table):
    high = table.astype(jnp.bfloat16)
    low = (table - high.astype(np.float32)).astype(jnp.bfloat16)
    return high, low


def tables(size_y, size_z):
    freq, place = np.arange(4)[:, None], np.arange(4)[None, :]
    scale = np.where(freq == 0, 0.5, np.sqrt(0.5))
    dct = scale * np.cos(np.pi * (2.0 * place + 1.0) * freq / 8.0)
    dz = np.kron(np.eye(size_z // 4), dct).astype(np.float32)
    dxy = np.kron(dct, np.kron(np.eye(size_y // 4), dct)).T.astype(np.float32)
    taps = {k: STAR[k] for k in range(1, 5)}
    inner = np.zeros((size_z, size_z), np.float32)
    halo = np.zeros((8, size_z), np.float32)
    for lane in range(size_z):
        for k, c in taps.items():
            for at in (lane + k, lane - k):
                if 0 <= at < size_z:
                    inner[at, lane] += c
                elif at < 0:
                    halo[4 + at, lane] += c
                else:
                    halo[4 + at - size_z, lane] += c
    pick = np.zeros((8, size_z), np.float32)
    for j in range(4):
        pick[j, j] = 1.0
        pick[4 + j, size_z - 4 + j] = 1.0
    dz_h, dz_l = halves_np(dz)
    dxy_h, dxy_l = halves_np(dxy)
    in_h, in_l = halves_np(inner)
    ha_h, ha_l = halves_np(halo)
    pick = pick.astype(jnp.bfloat16)
    spread = np.kron(np.eye(size_z // 4), np.ones((1, 4))).astype(jnp.bfloat16)
    repeat = np.kron(np.eye(size_y // 4), np.ones((4, 1)))
    return (
        np.concatenate([dz_h, dz_h, dz_l], 0),
        np.concatenate([dxy_h, dxy_h, dxy_l], 1),
        np.concatenate([in_h, in_h, in_l], 0),
        np.concatenate([ha_h, ha_h, ha_l, 0 * ha_l], 0),
        np.concatenate([pick, pick], 1),
        spread,
        repeat,
    )


def halves(value):
    high = value.astype(BF16)
    low = (value - high.astype(F32)).astype(BF16)
    return high, low


def dot(a, b, dims=((1,), (0,))):
    return lax.dot_general(a, b, (dims, ((), ())), preferred_element_type=F32)


def kernel(shape, steps, ntab, *refs):
    size_x, size_y, size_z = shape
    rows = size_x * size_y
    groups = size_x // 4
    ins, refs = refs[:8 + ntab], refs[8 + ntab:]
    outs, refs = refs[:3], refs[3:]
    vins, refs = refs[:8 + ntab], refs[8 + ntab:]
    (F, X, Y, ZS, ZR, Z, J, INV, B, A, T, LF, isem, ssem, rsem) = refs
    G, LAST, BEFORE = outs
    coef_v, keep_v, cour_v, damp_v, next_v, _, cell_v, data_v = vins[:8]
    dz_v, dxy_v, in_v, ha_v, pick_v, spread_v, repeat_v = vins[8:]
    pos = [lax.axis_index(a) for a in AXES]
    num = [lax.axis_size(a) for a in AXES]
    below = [p > 0 for p in pos]
    above = [p < n - 1 for p, n in zip(pos, num)]
    body = (pl.ds(PADX, size_x), pl.ds(PADY, size_y))

    order = [5, 3, 2, 4] + list(range(8, 8 + ntab)) + [6, 7, 1, 0]
    loads = {}
    for i in order:
        dst = F.at[(0,) + body] if i == 5 else vins[i]
        loads[i] = pltpu.make_async_copy(ins[i], dst, isem.at[i])
        loads[i].start()

    barrier = pltpu.get_barrier_semaphore()
    total = jnp.int32(0)
    for d, axis in enumerate(AXES):
        for has, to in ((above[d], pos[d] + 1), (below[d], pos[d] - 1)):
            total = total + has.astype(jnp.int32)

            @pl.when(has)
            def _(axis=axis, to=to):
                pl.semaphore_signal(barrier, inc=1, device_id={axis: to}, device_id_type=MESH)

    F[:, :, pl.ds(0, PADY), :] = jnp.zeros((2 * steps, size_x + 8, PADY, size_z), F32)
    F[:, :, pl.ds(PADY + size_y, PADY), :] = jnp.zeros((2 * steps, size_x + 8, PADY, size_z), F32)
    F[:, pl.ds(0, PADX), pl.ds(PADY, size_y), :] = jnp.zeros((2 * steps, PADX, size_y, size_z), F32)
    F[:, pl.ds(PADX + size_x, PADX), pl.ds(PADY, size_y), :] = jnp.zeros((2 * steps, PADX, size_y, size_z), F32)
    Y[:, 0, :, pl.ds(8, 8), :] = jnp.zeros((2 * steps, size_x, 8, size_z), F32)
    Y[:, 1, :, pl.ds(0, 8), :] = jnp.zeros((2 * steps, size_x, 8, size_z), F32)
    for side, has in ((0, below), (1, above)):

        @pl.when(jnp.logical_not(has[0]))
        def _(side=side):
            X[:, side] = jnp.zeros((2 * steps, 4, size_y, size_z), F32)

        @pl.when(jnp.logical_not(has[1]))
        def _(side=side):
            Y[:, side, :, pl.ds(4 + 4 * side, 4), :] = jnp.zeros((2 * steps, size_x, 4, size_z), F32)

        @pl.when(jnp.logical_not(has[2]))
        def _(side=side):
            ZR[:, side] = jnp.zeros((2 * steps, 4, rows), F32)

    def copy_of(r, d):
        axis, up = AXES[d // 2], d % 2 == 0
        if d == 0:
            src, dst = F.at[r, pl.ds(PADX + size_x - 4, 4), pl.ds(PADY, size_y)], X.at[r, 0]
        elif d == 1:
            src, dst = F.at[r, pl.ds(PADX, 4), pl.ds(PADY, size_y)], X.at[r, 1]
        elif d == 2:
            src = F.at[r, pl.ds(PADX, size_x), pl.ds(PADY + size_y - 4, 4)]
            dst = Y.at[r, 0, :, pl.ds(4, 4)]
        elif d == 3:
            src, dst = F.at[r, pl.ds(PADX, size_x), pl.ds(PADY, 4)], Y.at[r, 1, :, pl.ds(8, 4)]
        elif d == 4:
            src, dst = ZS.at[r, 1], ZR.at[r, 0]
        else:
            src, dst = ZS.at[r, 0], ZR.at[r, 1]
        to = pos[d // 2] + (1 if up else -1)
        return pltpu.make_async_remote_copy(
            src_ref=src, dst_ref=dst, send_sem=ssem.at[r, d], recv_sem=rsem.at[r, d],
            device_id={axis: to}, device_id_type=MESH,
        )

    def goes(d):
        return above[d // 2] if d % 2 == 0 else below[d // 2]

    def comes(d):
        return below[d // 2] if d % 2 == 0 else above[d // 2]

    def send(r, ds):
        for d in ds:

            @pl.when(goes(d))
            def _(d=d):
                copy_of(r, d).start()

    def arrive(r):
        for d in range(6):

            @pl.when(comes(d))
            def _(d=d):
                copy_of(r, d).wait_recv()

    def split_field(r):
        parts = [F[r, PADX + x, pl.ds(PADY, size_y), :] for x in range(size_x)]
        return halves(jnp.concatenate(parts, 0))

    def pack(r, high, low):
        packed = dot(pick_v[...], jnp.concatenate([high, low], 1), ((1,), (1,)))
        ZS[r, 0] = packed[0:4]
        ZS[r, 1] = packed[4:8]

    def inner_z(high, low):
        Z[...] = dot(jnp.concatenate([high, low, high], 1), in_v[...])

    def planes(fun, unit=2):
        def trip(i, carry):
            for j in range(unit):
                fun(i * unit + j)
            return carry

        lax.fori_loop(0, size_x // unit, trip, 0)

    def star(r, x):
        centre = pl.ds(PADY, size_y)
        out = 3.0 * STAR[0] * F[r, PADX + x, centre, :]
        for k in range(1, 5):
            out += STAR[k] * (
                (F[r, PADX + x + k, centre, :] + F[r, PADX + x - k, centre, :])
                + (F[r, PADX + x, pl.ds(PADY + k, size_y), :] + F[r, PADX + x, pl.ds(PADY - k, size_y), :])
            )
        return out + Z[pl.ds(pl.multiple_of(x * size_y, size_y), size_y), :]

    def halo_z(r):
        high, low = halves(jnp.concatenate([ZR[r, 0], ZR[r, 1]], 0).T)
        stacked = jnp.concatenate([high, low, high, jnp.zeros_like(low)], 1)
        Z[...] = dot(stacked, ha_v[...])

    def halo(r, x):
        out = Z[pl.ds(x * size_y, size_y), :]
        for k in range(1, 5):
            if x - k < 0:
                out += STAR[k] * X[r, 0, 4 + x - k]
            if x + k >= size_x:
                out += STAR[k] * X[r, 1, x + k - size_x]
        first = sum(STAR[k] * Y[r, 0, x, pl.ds(8 - k, 8), :] for k in range(1, 5))
        final = sum(STAR[k] * Y[r, 1, x, pl.ds(k, 8), :] for k in range(1, 5))
        return jnp.concatenate([out[0:8] + first, out[8:size_y - 8], out[size_y - 8:] + final], 0)

    cell = []

    def inject(s):
        if not cell:
            loads[6].wait()
            loads[7].wait()
        shift = size_z.bit_length() - 1
        at = cell_v[...]
        row = lax.shift_right_logical(at, jnp.full_like(at, shift))
        lane = at & (size_z - 1)
        hot = jnp.where(lax.broadcasted_iota(jnp.int32, (size_z, at.shape[1]), 0) == lane, 1.0, 0.0).astype(BF16)
        cell.append(1)
        spot = jnp.where(lax.broadcasted_iota(jnp.int32, (rows, at.shape[1]), 0) == row, data_v[pl.ds(s, 1), :], 0.0)
        high, low = halves(spot)
        J[...] = dot(jnp.concatenate([high, low], 1), jnp.concatenate([hot, hot], 1), ((1,), (1,)))

    def before_halo(s):
        def one(x):
            lap = star(s, x)
            later = next_v[x] if s == 0 else F[s - 1, PADX + x, pl.ds(PADY, size_y), :]
            got = J[pl.ds(pl.multiple_of(x * size_y, size_y), size_y), :]
            value = 2.0 * F[s, PADX + x, pl.ds(PADY, size_y), :] - (1.0 - damp_v[x]) * later + got
            A[x] = INV[x] * value + B[x] * lap

        planes(one)

    def after_halo(s):
        halo_z(s)
        for x in range(size_x):
            value = A[x] + B[x] * halo(s, x)
            if s == steps - 1:
                LAST[x] = value
            else:
                F[s + 1, PADX + x, pl.ds(PADY, size_y), :] = value
            if s == steps - 2:
                BEFORE[x] = value

    def mask_setup():
        loads[1].wait()
        wide = dot(keep_v[...].astype(F32).astype(BF16), spread_v[...])
        sub = lax.broadcasted_iota(jnp.int32, (size_y, size_z), 0) % 4
        lan = lax.broadcasted_iota(jnp.int32, (size_y, size_z), 1) % 4
        level = (sub + lan).astype(F32)
        per = size_y // 4
        for g in range(steps * groups):
            T[g] = dot(repeat_v[...], wide[g * per:(g + 1) * per].astype(BF16)) - level

    def decode(s):
        r = steps + s
        parts = []
        for g in range(groups):
            limit = T[s * groups + g]
            for a in range(4):
                block = coef_v[s, g * 4 + a]
                parts.append(jnp.where(limit > float(a), block, 0.0))
        high, low = halves(jnp.concatenate(parts, 0))
        along = dot(jnp.concatenate([high, low, high], 1), dz_v[...])
        high, low = halves(along)
        span = 4 * size_y
        hs = jnp.concatenate([high[g * span:(g + 1) * span] for g in range(groups)], 1)
        ls = jnp.concatenate([low[g * span:(g + 1) * span] for g in range(groups)], 1)
        out = dot(dxy_v[...], jnp.concatenate([hs, ls, hs], 0))
        for g in range(groups):
            for a in range(4):
                F[r, PADX + 4 * g + a, pl.ds(PADY, size_y), :] = out[
                    a * size_y:(a + 1) * size_y, g * size_z:(g + 1) * size_z
                ]
        send(r, (0, 1, 2, 3))
        pack(r, *split_field(r))
        send(r, (4, 5))

    def gradient(s):
        r = steps + s
        inner_z(*split_field(r))

        def one(x):
            LF[x] = star(r, x)

        planes(one)
        arrive(r)
        halo_z(r)
        for x in range(size_x):
            term = cour_v[x] * F[s, PADX + x, pl.ds(PADY, size_y), :] * (LF[x] + halo(r, x))
            G[x] = term if s == 0 else G[x] + term

    def setup_scales():
        loads[2].wait()
        loads[3].wait()

        def one(x):
            inverse = 1.0 / (1.0 + damp_v[x])
            INV[x] = inverse
            B[x] = cour_v[x] * inverse

        planes(one)

    for i in (5,) + tuple(range(8, 8 + ntab)):
        loads[i].wait()
    high, low = split_field(0)
    pack(0, high, low)
    pl.semaphore_wait(barrier, total)
    send(0, range(6))
    for s in range(steps):
        inner_z(high, low)
        inject(s)
        if s == 0:
            setup_scales()
            loads[4].wait()
        before_halo(s)
        if s == 0:
            mask_setup()
            loads[0].wait()
        for t in (2 * s, 2 * s + 1):
            if t < steps:
                decode(t)
            elif t < 2 * steps:
                gradient(t - steps)
        arrive(s)
        after_halo(s)
        if s < steps - 1:
            send(s + 1, (0, 1, 2, 3))
            high, low = split_field(s + 1)
            pack(s + 1, high, low)
            send(s + 1, (4, 5))
    for r in range(2 * steps):
        for d in range(6):

            @pl.when(goes(d))
            def _(r=r, d=d):
                copy_of(r, d).wait_send()


def flush(*refs):
    sources, targets, sem = refs[:3], refs[3:6], refs[6]
    copies = [pltpu.make_async_copy(a, b, sem.at[i]) for i, (a, b) in enumerate(zip(sources, targets))]
    for c in copies:
        c.start()
    for c in copies:
        c.wait()


def local(coef, keep, courant, damp, adj_next, adj_now, rec_cell, rec_data):
    shape = adj_now.shape
    size_x, size_y, size_z = shape
    steps = coef.shape[0]
    rows = size_x * size_y
    args = [
        coef, keep.reshape(-1, keep.shape[-1]), courant, damp, adj_next, adj_now,
        rec_cell.reshape(1, -1), rec_data.reshape(steps, -1),
    ]
    tabs = list(tables(size_y, size_z))
    tabs[-1] = tabs[-1].astype(jnp.bfloat16)
    tabs = [jnp.asarray(t) for t in tabs]
    args += tabs
    box = pltpu.VMEM(shape, F32)
    flat = pltpu.VMEM((rows, size_z), F32)
    scratch = [pltpu.VMEM(a.shape, a.dtype) for a in args]
    scratch[5] = pltpu.VMEM((8, 128), F32)
    scratch += [
        pltpu.VMEM((2 * steps, size_x + 8, size_y + 16, size_z), F32),
        pltpu.VMEM((2 * steps, 2, 4, size_y, size_z), F32),
        pltpu.VMEM((2 * steps, 2, size_x, 16, size_z), F32),
        pltpu.VMEM((2 * steps, 2, 4, rows), F32),
        pltpu.VMEM((2 * steps, 2, 4, rows), F32),
        flat, flat, box, box, box,
        pltpu.VMEM((steps * size_x // 4, size_y, size_z), F32),
        box,
        pltpu.SemaphoreType.DMA((len(args),)),
        pltpu.SemaphoreType.DMA((2 * steps, 6)),
        pltpu.SemaphoreType.DMA((2 * steps, 6)),
    ]
    hbm = pl.BlockSpec(memory_space=pl.ANY)
    args = [pltpu.with_memory_space_constraint(a, pltpu.HBM) for a in args]
    results = pl.pallas_call(
        functools.partial(kernel, shape, steps, len(tabs)),
        out_shape=[jax.ShapeDtypeStruct(shape, F32)] * 3,
        in_specs=[hbm] * len(args),
        out_specs=[pl.BlockSpec(memory_space=pltpu.VMEM)] * 3,
        scratch_shapes=scratch,
        compiler_params=pltpu.CompilerParams(
            collective_id=0, has_side_effects=True, vmem_limit_bytes=48 * 2**20
        ),
    )(*args)
    return tuple(pl.pallas_call(
        flush,
        out_shape=[jax.ShapeDtypeStruct(shape, F32)] * 3,
        in_specs=[hbm] * 3,
        out_specs=[hbm] * 3,
        scratch_shapes=[pltpu.SemaphoreType.DMA((3,))],
        compiler_params=pltpu.CompilerParams(vmem_limit_bytes=2**20),
    )(*results))


def solution(mesh):
    in_specs = (
        P(None, "gx", "gy", "gz"),
        P(None, "gx", "gy", "gz"),
        P("gx", "gy", "gz"),
        P("gx", "gy", "gz"),
        P("gx", "gy", "gz"),
        P("gx", "gy", "gz"),
        P("gx", "gy", "gz", None),
        P("gx", "gy", "gz", None, None),
    )
    out_specs = (P("gx", "gy", "gz"), P("gx", "gy", "gz"), P("gx", "gy", "gz"))
    return jax.shard_map(local, mesh=mesh, in_specs=in_specs, out_specs=out_specs, check_vma=False)
```

```python
import functools

import jax
import jax.numpy as jnp
import numpy as np
from jax import lax
from jax.experimental import pallas as pl
from jax.experimental.pallas import tpu as pltpu
from jax.sharding import PartitionSpec as P

STAR = (-205.0 / 72.0, 8.0 / 5.0, -1.0 / 5.0, 8.0 / 315.0, -1.0 / 560.0)
MESH = pl.DeviceIdType.MESH
F32, BF16 = jnp.float32, jnp.bfloat16
AXES = ("gx", "gy", "gz")
PADX, PADY = 4, 8


def halves_np(table):
    high = table.astype(jnp.bfloat16)
    low = (table - high.astype(np.float32)).astype(jnp.bfloat16)
    return high, low


def tables(size_y, size_z):
    freq, place = np.arange(4)[:, None], np.arange(4)[None, :]
    scale = np.where(freq == 0, 0.5, np.sqrt(0.5))
    dct = scale * np.cos(np.pi * (2.0 * place + 1.0) * freq / 8.0)
    dz = np.kron(np.eye(size_z // 4), dct).astype(np.float32)
    dxy = np.kron(dct, np.kron(np.eye(size_y // 4), dct)).T.astype(np.float32)
    taps = {k: STAR[k] for k in range(1, 5)}
    inner = np.zeros((size_z, size_z), np.float32)
    halo = np.zeros((8, size_z), np.float32)
    for lane in range(size_z):
        for k, c in taps.items():
            for at in (lane + k, lane - k):
                if 0 <= at < size_z:
                    inner[at, lane] += c
                elif at < 0:
                    halo[4 + at, lane] += c
                else:
                    halo[4 + at - size_z, lane] += c
    pick = np.zeros((8, size_z), np.float32)
    for j in range(4):
        pick[j, j] = 1.0
        pick[4 + j, size_z - 4 + j] = 1.0
    dz_h, dz_l = halves_np(dz)
    dxy_h, dxy_l = halves_np(dxy)
    in_h, in_l = halves_np(inner)
    ha_h, ha_l = halves_np(halo)
    pick = pick.astype(jnp.bfloat16)
    spread = np.kron(np.eye(size_z // 4), np.ones((1, 4))).astype(jnp.bfloat16)
    repeat = np.kron(np.eye(size_y // 4), np.ones((4, 1)))
    return (
        np.concatenate([dz_h, dz_h, dz_l], 0),
        np.concatenate([dxy_h, dxy_h, dxy_l], 1),
        np.concatenate([in_h, in_h, in_l], 0),
        np.concatenate([ha_h, ha_h, ha_l, 0 * ha_l], 0),
        np.concatenate([pick, pick], 1),
        spread,
        repeat,
    )


def halves(value):
    high = value.astype(BF16)
    low = (value - high.astype(F32)).astype(BF16)
    return high, low


def dot(a, b, dims=((1,), (0,))):
    return lax.dot_general(a, b, (dims, ((), ())), preferred_element_type=F32)


def kernel(shape, steps, ntab, *refs):
    size_x, size_y, size_z = shape
    rows = size_x * size_y
    groups = size_x // 4
    ins, refs = refs[:8 + ntab], refs[8 + ntab:]
    outs, refs = refs[:3], refs[3:]
    vins, refs = refs[:8 + ntab], refs[8 + ntab:]
    (F, X, Y, ZS, ZR, Z, J, INV, B, A, T, LF, isem, ssem, rsem) = refs
    G, LAST, BEFORE = outs
    coef_v, keep_v, cour_v, damp_v, next_v, _, cell_v, data_v = vins[:8]
    dz_v, dxy_v, in_v, ha_v, pick_v, spread_v, repeat_v = vins[8:]
    pos = [lax.axis_index(a) for a in AXES]
    num = [lax.axis_size(a) for a in AXES]
    below = [p > 0 for p in pos]
    above = [p < n - 1 for p, n in zip(pos, num)]
    body = (pl.ds(PADX, size_x), pl.ds(PADY, size_y))

    order = [5, 3, 2, 4] + list(range(8, 8 + ntab)) + [6, 7, 1, 0]
    loads = {}
    for i in order:
        dst = F.at[(0,) + body] if i == 5 else vins[i]
        loads[i] = pltpu.make_async_copy(ins[i], dst, isem.at[i])
        loads[i].start()

    barrier = pltpu.get_barrier_semaphore()
    total = jnp.int32(0)
    for d, axis in enumerate(AXES):
        for has, to in ((above[d], pos[d] + 1), (below[d], pos[d] - 1)):
            total = total + has.astype(jnp.int32)

            @pl.when(has)
            def _(axis=axis, to=to):
                pl.semaphore_signal(barrier, inc=1, device_id={axis: to}, device_id_type=MESH)

    F[:, :, pl.ds(0, PADY), :] = jnp.zeros((2 * steps, size_x + 8, PADY, size_z), F32)
    F[:, :, pl.ds(PADY + size_y, PADY), :] = jnp.zeros((2 * steps, size_x + 8, PADY, size_z), F32)
    F[:, pl.ds(0, PADX), pl.ds(PADY, size_y), :] = jnp.zeros((2 * steps, PADX, size_y, size_z), F32)
    F[:, pl.ds(PADX + size_x, PADX), pl.ds(PADY, size_y), :] = jnp.zeros((2 * steps, PADX, size_y, size_z), F32)
    Y[:, 0, :, pl.ds(8, 8), :] = jnp.zeros((2 * steps, size_x, 8, size_z), F32)
    Y[:, 1, :, pl.ds(0, 8), :] = jnp.zeros((2 * steps, size_x, 8, size_z), F32)
    for side, has in ((0, below), (1, above)):

        @pl.when(jnp.logical_not(has[0]))
        def _(side=side):
            X[:, side] = jnp.zeros((2 * steps, 4, size_y, size_z), F32)

        @pl.when(jnp.logical_not(has[1]))
        def _(side=side):
            Y[:, side, :, pl.ds(4 + 4 * side, 4), :] = jnp.zeros((2 * steps, size_x, 4, size_z), F32)

        @pl.when(jnp.logical_not(has[2]))
        def _(side=side):
            ZR[:, side] = jnp.zeros((2 * steps, 4, rows), F32)

    def copy_of(r, d):
        axis, up = AXES[d // 2], d % 2 == 0
        if d == 0:
            src, dst = F.at[r, pl.ds(PADX + size_x - 4, 4), pl.ds(PADY, size_y)], X.at[r, 0]
        elif d == 1:
            src, dst = F.at[r, pl.ds(PADX, 4), pl.ds(PADY, size_y)], X.at[r, 1]
        elif d == 2:
            src = F.at[r, pl.ds(PADX, size_x), pl.ds(PADY + size_y - 4, 4)]
            dst = Y.at[r, 0, :, pl.ds(4, 4)]
        elif d == 3:
            src, dst = F.at[r, pl.ds(PADX, size_x), pl.ds(PADY, 4)], Y.at[r, 1, :, pl.ds(8, 4)]
        elif d == 4:
            src, dst = ZS.at[r, 1], ZR.at[r, 0]
        else:
            src, dst = ZS.at[r, 0], ZR.at[r, 1]
        to = pos[d // 2] + (1 if up else -1)
        return pltpu.make_async_remote_copy(
            src_ref=src, dst_ref=dst, send_sem=ssem.at[r, d], recv_sem=rsem.at[r, d],
            device_id={axis: to}, device_id_type=MESH,
        )

    def goes(d):
        return above[d // 2] if d % 2 == 0 else below[d // 2]

    def comes(d):
        return below[d // 2] if d % 2 == 0 else above[d // 2]

    def send(r, ds):
        for d in ds:

            @pl.when(goes(d))
            def _(d=d):
                copy_of(r, d).start()

    def arrive(r, ds=range(6)):
        for d in ds:

            @pl.when(comes(d))
            def _(d=d):
                copy_of(r, d).wait_recv()

    def split_field(r):
        parts = [F[r, PADX + x, pl.ds(PADY, size_y), :] for x in range(size_x)]
        return halves(jnp.concatenate(parts, 0))

    def pack(r, high, low):
        packed = dot(pick_v[...], jnp.concatenate([high, low], 1), ((1,), (1,)))
        ZS[r, 0] = packed[0:4]
        ZS[r, 1] = packed[4:8]

    def inner_z(high, low):
        Z[...] = dot(jnp.concatenate([high, low, high], 1), in_v[...])

    def planes(fun, unit=2):
        def trip(i, carry):
            for j in range(unit):
                fun(i * unit + j)
            return carry

        lax.fori_loop(0, size_x // unit, trip, 0)

    def star(r, x):
        centre = pl.ds(PADY, size_y)
        out = 3.0 * STAR[0] * F[r, PADX + x, centre, :]
        for k in range(1, 5):
            out += STAR[k] * (
                (F[r, PADX + x + k, centre, :] + F[r, PADX + x - k, centre, :])
                + (F[r, PADX + x, pl.ds(PADY + k, size_y), :] + F[r, PADX + x, pl.ds(PADY - k, size_y), :])
            )
        return out + Z[pl.ds(pl.multiple_of(x * size_y, size_y), size_y), :]

    def halo_z(r):
        faces = jnp.concatenate([ZR[r, 0], ZR[r, 1]], 0)
        high = faces.astype(BF16).astype(F32)
        stacked = jnp.concatenate([high, faces - high, high, jnp.zeros_like(high)], 0)
        Z[...] = dot(stacked.astype(BF16), ha_v[...], ((0,), (0,)))

    def halo(r, x):
        out = Z[pl.ds(x * size_y, size_y), :]
        for k in range(1, 5):
            if x - k < 0:
                out += STAR[k] * X[r, 0, 4 + x - k]
            if x + k >= size_x:
                out += STAR[k] * X[r, 1, x + k - size_x]
        first = sum(STAR[k] * Y[r, 0, x, pl.ds(8 - k, 8), :] for k in range(1, 5))
        final = sum(STAR[k] * Y[r, 1, x, pl.ds(k, 8), :] for k in range(1, 5))
        return jnp.concatenate([out[0:8] + first, out[8:size_y - 8], out[size_y - 8:] + final], 0)

    cell = []

    def inject(s):
        if not cell:
            loads[6].wait()
            loads[7].wait()
        shift = size_z.bit_length() - 1
        at = cell_v[...]
        row = lax.shift_right_logical(at, jnp.full_like(at, shift))
        lane = at & (size_z - 1)
        hot = jnp.where(lax.broadcasted_iota(jnp.int32, (size_z, at.shape[1]), 0) == lane, 1.0, 0.0).astype(BF16)
        cell.append(1)
        spot = jnp.where(lax.broadcasted_iota(jnp.int32, (rows, at.shape[1]), 0) == row, data_v[pl.ds(s, 1), :], 0.0)
        high, low = halves(spot)
        J[...] = dot(jnp.concatenate([high, low], 1), jnp.concatenate([hot, hot], 1), ((1,), (1,)))

    def before_halo(s):
        def one(x):
            lap = star(s, x)
            later = next_v[x] if s == 0 else F[s - 1, PADX + x, pl.ds(PADY, size_y), :]
            got = J[pl.ds(pl.multiple_of(x * size_y, size_y), size_y), :]
            value = 2.0 * F[s, PADX + x, pl.ds(PADY, size_y), :] - (1.0 - damp_v[x]) * later + got
            A[x] = INV[x] * value + B[x] * lap

        planes(one)

    def after_halo(s):
        arrive(s, (4, 5))
        halo_z(s)
        arrive(s, (0, 1, 2, 3))
        for x in range(size_x):
            value = A[x] + B[x] * halo(s, x)
            if s == steps - 1:
                LAST[x] = value
            else:
                F[s + 1, PADX + x, pl.ds(PADY, size_y), :] = value
            if s == steps - 2:
                BEFORE[x] = value

    def mask_setup():
        loads[1].wait()
        wide = dot(keep_v[...].astype(F32).astype(BF16), spread_v[...])
        sub = lax.broadcasted_iota(jnp.int32, (size_y, size_z), 0) % 4
        lan = lax.broadcasted_iota(jnp.int32, (size_y, size_z), 1) % 4
        level = (sub + lan).astype(F32)
        per = size_y // 4
        for g in range(steps * groups):
            T[g] = dot(repeat_v[...], wide[g * per:(g + 1) * per].astype(BF16)) - level

    def decode(s):
        r = steps + s
        parts = []
        for g in range(groups):
            limit = T[s * groups + g]
            for a in range(4):
                block = coef_v[s, g * 4 + a]
                parts.append(jnp.where(limit > float(a), block, 0.0))
        high, low = halves(jnp.concatenate(parts, 0))
        along = dot(jnp.concatenate([high, low, high], 1), dz_v[...])
        high, low = halves(along)
        span = 4 * size_y
        hs = jnp.concatenate([high[g * span:(g + 1) * span] for g in range(groups)], 1)
        ls = jnp.concatenate([low[g * span:(g + 1) * span] for g in range(groups)], 1)
        out = dot(dxy_v[...], jnp.concatenate([hs, ls, hs], 0))
        for g in range(groups):
            for a in range(4):
                F[r, PADX + 4 * g + a, pl.ds(PADY, size_y), :] = out[
                    a * size_y:(a + 1) * size_y, g * size_z:(g + 1) * size_z
                ]
        send(r, (0, 1, 2, 3))
        pack(r, *split_field(r))
        send(r, (4, 5))

    def gradient(s):
        r = steps + s
        inner_z(*split_field(r))

        def one(x):
            LF[x] = star(r, x)

        planes(one)
        arrive(r)
        halo_z(r)
        for x in range(size_x):
            term = cour_v[x] * F[s, PADX + x, pl.ds(PADY, size_y), :] * (LF[x] + halo(r, x))
            G[x] = term if s == 0 else G[x] + term

    def setup_scales():
        loads[2].wait()
        loads[3].wait()

        def one(x):
            inverse = 1.0 / (1.0 + damp_v[x])
            INV[x] = inverse
            B[x] = cour_v[x] * inverse

        planes(one)

    for i in (5,) + tuple(range(8, 8 + ntab)):
        loads[i].wait()
    high, low = split_field(0)
    pack(0, high, low)
    pl.semaphore_wait(barrier, total)
    send(0, range(6))
    for s in range(steps):
        inner_z(high, low)
        inject(s)
        if s == 0:
            setup_scales()
            loads[4].wait()
        before_halo(s)
        if s == 0:
            mask_setup()
            loads[0].wait()
        for t in (2 * s, 2 * s + 1):
            if t < steps:
                decode(t)
            elif t < 2 * steps:
                gradient(t - steps)
        after_halo(s)
        if s < steps - 1:
            high, low = split_field(s + 1)
            pack(s + 1, high, low)
            send(s + 1, range(6))
    for r in range(2 * steps):
        for d in range(6):

            @pl.when(goes(d))
            def _(r=r, d=d):
                copy_of(r, d).wait_send()


def flush(*refs):
    sources, targets, sem = refs[:3], refs[3:6], refs[6]
    copies = [pltpu.make_async_copy(a, b, sem.at[i]) for i, (a, b) in enumerate(zip(sources, targets))]
    for c in copies:
        c.start()
    for c in copies:
        c.wait()


def local(coef, keep, courant, damp, adj_next, adj_now, rec_cell, rec_data):
    shape = adj_now.shape
    size_x, size_y, size_z = shape
    steps = coef.shape[0]
    rows = size_x * size_y
    args = [
        coef, keep.reshape(-1, keep.shape[-1]), courant, damp, adj_next, adj_now,
        rec_cell.reshape(1, -1), rec_data.reshape(steps, -1),
    ]
    tabs = list(tables(size_y, size_z))
    tabs[-1] = tabs[-1].astype(jnp.bfloat16)
    tabs = [jnp.asarray(t) for t in tabs]
    args += tabs
    box = pltpu.VMEM(shape, F32)
    flat = pltpu.VMEM((rows, size_z), F32)
    scratch = [pltpu.VMEM(a.shape, a.dtype) for a in args]
    scratch[5] = pltpu.VMEM((8, 128), F32)
    scratch += [
        pltpu.VMEM((2 * steps, size_x + 8, size_y + 16, size_z), F32),
        pltpu.VMEM((2 * steps, 2, 4, size_y, size_z), F32),
        pltpu.VMEM((2 * steps, 2, size_x, 16, size_z), F32),
        pltpu.VMEM((2 * steps, 2, 4, rows), F32),
        pltpu.VMEM((2 * steps, 2, 4, rows), F32),
        flat, flat, box, box, box,
        pltpu.VMEM((steps * size_x // 4, size_y, size_z), F32),
        box,
        pltpu.SemaphoreType.DMA((len(args),)),
        pltpu.SemaphoreType.DMA((2 * steps, 6)),
        pltpu.SemaphoreType.DMA((2 * steps, 6)),
    ]
    hbm = pl.BlockSpec(memory_space=pl.ANY)
    args = [pltpu.with_memory_space_constraint(a, pltpu.HBM) for a in args]
    results = pl.pallas_call(
        functools.partial(kernel, shape, steps, len(tabs)),
        out_shape=[jax.ShapeDtypeStruct(shape, F32)] * 3,
        in_specs=[hbm] * len(args),
        out_specs=[pl.BlockSpec(memory_space=pltpu.VMEM)] * 3,
        scratch_shapes=scratch,
        compiler_params=pltpu.CompilerParams(
            collective_id=0, has_side_effects=True, vmem_limit_bytes=48 * 2**20
        ),
    )(*args)
    return tuple(pl.pallas_call(
        flush,
        out_shape=[jax.ShapeDtypeStruct(shape, F32)] * 3,
        in_specs=[hbm] * 3,
        out_specs=[hbm] * 3,
        scratch_shapes=[pltpu.SemaphoreType.DMA((3,))],
        compiler_params=pltpu.CompilerParams(vmem_limit_bytes=2**20),
    )(*results))


def solution(mesh):
    in_specs = (
        P(None, "gx", "gy", "gz"),
        P(None, "gx", "gy", "gz"),
        P("gx", "gy", "gz"),
        P("gx", "gy", "gz"),
        P("gx", "gy", "gz"),
        P("gx", "gy", "gz"),
        P("gx", "gy", "gz", None),
        P("gx", "gy", "gz", None, None),
    )
    out_specs = (P("gx", "gy", "gz"), P("gx", "gy", "gz"), P("gx", "gy", "gz"))
    return jax.shard_map(local, mesh=mesh, in_specs=in_specs, out_specs=out_specs, check_vma=False)
```
